128 devices in a mesh: tok: 8 (over z, core), seq: 16 (over y, x).
Axes of the slice: x: 4, y: 4, z: 4, core: 2. Of those that a mesh axis runs over, the one named last changes fastest.
Arguments:
- keys: bfloat16 [16, 2, 8192, 512], P('seq', None, 'tok'), may hold values from -6 to 6
- values: bfloat16 [16, 2, 8192, 512], P('seq', None, 'tok'), may hold values from -6 to 6
- queries: bfloat16 [16, 2, 8192, 512], P('seq', None, 'tok'), may hold values from -6 to 6
- token_rate: float32 [16, 2, 8192], P('seq', None, 'tok'), may hold values from 0.1 to 1
- valid_count: int32 [16, 2], P('seq'), may hold values from 4096 to 8192
- loss_scale: float32 [1], replicated, may hold values from 128 to 2048
- w_gate: bfloat16 [512, 512], replicated, may hold values from -0.25 to 0.25
- w_up: bfloat16 [512, 512], replicated, may hold values from -0.25 to 0.25
- w_down: bfloat16 [512, 512], replicated, may hold values from -0.25 to 0.25
- out_cotangent: bfloat16 [16, 2, 8192, 512], P('seq', None, 'tok'), may hold values from -0.0625 to 0.0625
Outputs:
- fast_out: bfloat16 [16, 2, 8192, 512], P('seq', None, 'tok')
- grad_gate: float32 [512, 512], P(None, 'tok')
- grad_up: float32 [512, 512], P(None, 'tok')
- grad_down: float32 [512, 512], P('tok')
- levels: float32 [2, 512], P(None, 'tok')
The draws below stay inside these ranges and needn't reach their ends.
All inputs are finite; a program needn't handle non-finite values.
Results may differ from the reference program's by a relative error of at most 0.0087.
Values may be sent and summed in bfloat16 or wider, within the bound.
No kernel may reach another device: no remote copies, remote signals or barrier semaphores. Data moves between devices by JAX's collectives and lax.ppermute only.
A program may use at most 128 MiB of HBM per device.

```python
import math
import jax
import jax.numpy as jnp
from jax import lax

D = 512
HID = 512
BLOCKS = 2
BLOCK_LEN = 8192
SEQS = 16
ALL_TOKENS = 262144


def with_ends(array, own_key, least, largest):
    longest = array.shape.index(max(array.shape))
    spots = []
    for shift in (0, 1):
        where = [jax.random.randint(jax.random.fold_in(own_key, axis), (), 0, length) for axis, length in enumerate(array.shape)]
        where[longest] = (where[longest] + shift) % array.shape[longest]
        spots.append(tuple(where))
    return array.at[spots[0]].set(least).at[spots[1]].set(largest)


def steps_of(rng, extent, pieces, low, high):
    factor_of = 1.0
    for dim, shards_of in pieces:
        heights = jax.random.uniform(jax.random.fold_in(jax.random.fold_in(rng, 6), dim), (shards_of,), jnp.float32, low / len(pieces), high / len(pieces))
        factor_of = factor_of * jnp.repeat(jnp.exp(heights), extent[dim] // shards_of).reshape((-1,) + (1,) * (len(extent) - 1 - dim))
    return factor_of


def scatter_about(rng, extent, spread, bound, cuts=(), kind=jnp.bfloat16):
    entries = jax.random.normal(rng, extent, jnp.float32) * spread
    if len(cuts) > 0:
        entries = steps_of(rng, extent, cuts, -0.22, 0.18) * entries
    return jnp.clip(entries, min=-bound, max=bound).astype(kind)


def setup_inputs(seed: int = 0) -> dict:
    key_list = jax.random.split(jax.random.key(seed), 11)
    keys = scatter_about(key_list[0], (SEQS, BLOCKS, BLOCK_LEN, D), 1.0, 6.0, ((0, 16), (2, 8)))
    values = scatter_about(key_list[1], (SEQS, BLOCKS, BLOCK_LEN, D), 1.0, 6.0, ((0, 16), (2, 8)))
    queries = scatter_about(key_list[2], (SEQS, BLOCKS, BLOCK_LEN, D), 1.0, 6.0, ((0, 16), (2, 8)))
    token_rate = jnp.clip(jnp.exp(math.log(1.0) - 2.3025851 * jax.random.uniform(key_list[3], (SEQS, BLOCKS, BLOCK_LEN), jnp.float32) ** steps_of(key_list[3], (SEQS, BLOCKS, BLOCK_LEN), ((0, 16), (2, 8)), -0.2, 0.2)), 0.1, 1.0)
    valid_count = with_ends(jax.random.randint(key_list[4], (SEQS, BLOCKS), BLOCK_LEN // 2, BLOCK_LEN + 1), jax.random.fold_in(key_list[4], 1), BLOCK_LEN // 2, BLOCK_LEN).astype(jnp.int32)
    loss_scale = jnp.clip(jnp.exp(jax.random.uniform(key_list[5], (1,), jnp.float32, math.log(128.0), math.log(2048.0))), 128.0, 2048.0)
    w_gate = scatter_about(key_list[6], (D, HID), D ** -0.5, 0.25)
    w_up = scatter_about(key_list[7], (D, HID), D ** -0.5, 0.25)
    w_down = scatter_about(key_list[8], (HID, D), HID ** -0.5, 0.25)
    out_cotangent = scatter_about(key_list[9], (SEQS, BLOCKS, BLOCK_LEN, D), (2.0 * ALL_TOKENS ** -0.5), 0.0625, ((0, 16), (2, 8)))
    return {"keys": keys, "values": values, "queries": queries, "token_rate": token_rate, "valid_count": valid_count, "loss_scale": loss_scale, "w_gate": w_gate, "w_up": w_up, "w_down": w_down, "out_cotangent": out_cotangent}


momentum_keep = 0.9
step_rate = 3.0
tiny_value = 1e-06

def forward(inputs, gate_w, up_w):
    gate = jnp.dot(inputs, gate_w, preferred_element_type=jnp.float32)
    upper = jnp.dot(inputs, up_w, preferred_element_type=jnp.float32)
    hidden = (jax.nn.silu(gate) * upper).astype(jnp.bfloat16)
    return (gate, upper, hidden)

def backward(inputs, gate, upper, hidden, down_w, cotan):
    grad_down = jnp.dot(hidden.T, cotan, preferred_element_type=jnp.float32)
    back = jnp.dot(cotan, down_w.T, preferred_element_type=jnp.float32)
    sigma = jax.nn.sigmoid(gate)
    d_upper = (back * gate * sigma).astype(jnp.bfloat16)
    d_gate = (back * upper * sigma * (1.0 + gate * (1.0 - sigma))).astype(jnp.bfloat16)
    grad_gate = jnp.dot(inputs.T, d_gate, preferred_element_type=jnp.float32)
    grad_up = jnp.dot(inputs.T, d_upper, preferred_element_type=jnp.float32)
    return (grad_gate, grad_up, grad_down)

def renorm(gate_w, up_w, down_w, gate_n, up_n, down_n):
    gate_w = gate_w * (gate_n / jnp.sqrt(lax.optimization_barrier(jnp.sum(gate_w * gate_w, axis=0)) + tiny_value))
    up_w = up_w * (up_n / jnp.sqrt(lax.optimization_barrier(jnp.sum(up_w * up_w, axis=0)) + tiny_value))
    down_w = down_w * (down_n / jnp.sqrt(lax.optimization_barrier(jnp.sum(down_w * down_w, axis=1)) + tiny_value))[:, None]
    return (gate_w, up_w, down_w)

def reference(keys, values, queries, token_rate, valid_count, loss_scale, w_gate, w_up, w_down, out_cotangent):
    scale = loss_scale[0]
    gate_full = w_gate.astype(jnp.float32)
    up_full = w_up.astype(jnp.float32)
    down_full = w_down.astype(jnp.float32)
    gate_n = jnp.sqrt(lax.optimization_barrier(jnp.sum(gate_full * gate_full, axis=0)) + tiny_value)
    up_n = jnp.sqrt(lax.optimization_barrier(jnp.sum(up_full * up_full, axis=0)) + tiny_value)
    down_n = jnp.sqrt(lax.optimization_barrier(jnp.sum(down_full * down_full, axis=1)) + tiny_value)
    positions = jnp.arange(BLOCK_LEN, dtype=jnp.int32)

    def one_sequence(items):
        key_seq, value_seq, query_seq, rate_seq, count_seq, cot_seq = items
        state = (gate_full, up_full, down_full)
        momentum = tuple((jnp.zeros_like(entry) for entry in state))
        totals = tuple((jnp.zeros_like(entry) for entry in state))
        current = (w_gate, w_up, w_down)
        level_list = []
        output_list = []
        for index in range(BLOCKS):
            count = count_seq[index]
            mask = (positions < count).astype(jnp.float32)
            inputs = key_seq[index]
            gate, upper, hidden = forward(inputs, current[0], current[1])
            factor = -(scale * rate_seq[index] * mask / count.astype(jnp.float32))
            cotan = (factor[:, None] * value_seq[index].astype(jnp.float32)).astype(jnp.bfloat16)
            summed = backward(inputs, gate, upper, hidden, current[2], cotan)
            level_list.append(lax.optimization_barrier(jnp.max(jnp.abs(summed[0]), axis=0)))
            momentum = tuple((momentum_keep * held + grad / scale for held, grad in zip(momentum, summed)))
            stepped = tuple((entry - step_rate * held for entry, held in zip(state, momentum)))
            state = renorm(stepped[0], stepped[1], stepped[2], gate_n, up_n, down_n)
            current = tuple((entry.astype(jnp.bfloat16) for entry in state))
            inputs = query_seq[index]
            gate, upper, hidden = forward(inputs, current[0], current[1])
            result = jnp.dot(hidden, current[2], preferred_element_type=jnp.float32)
            output_list.append((result * mask[:, None]).astype(jnp.bfloat16))
            outer_cot = cot_seq[index] * mask[:, None].astype(jnp.bfloat16)
            partial_grads = backward(inputs, gate, upper, hidden, current[2], outer_cot)
            totals = tuple((held + grad for held, grad in zip(totals, partial_grads)))
        return (jnp.stack(output_list), totals[0], totals[1], totals[2], jnp.stack(level_list))
    results = lax.map(one_sequence, (keys, values, queries, token_rate, valid_count, out_cotangent))
    fast_out = results[0]
    grad_gate = lax.optimization_barrier(jnp.sum(results[1], axis=0))
    grad_up = lax.optimization_barrier(jnp.sum(results[2], axis=0))
    grad_down = lax.optimization_barrier(jnp.sum(results[3], axis=0))
    levels = lax.optimization_barrier(jnp.max(results[4], axis=0))
    return (fast_out, grad_gate, grad_up, grad_down, levels)
```

```python
import functools
import jax
import jax.numpy as jnp
from jax import lax
from jax.experimental import pallas as pl
from jax.experimental.pallas import tpu as pltpu
from jax.sharding import PartitionSpec as P

KEEP = 0.9
RATE = 3.0
TINY = 1e-06
BF = jnp.bfloat16
F32 = jnp.float32
NT = (((1,), (1,)), ((), ()))
TN = (((0,), (0,)), ((), ()))
VMEM_LIMIT = 56 * 1024 * 1024


def dot(a, b, dims=None):
    if dims is None:
        return jnp.dot(a, b, preferred_element_type=F32)
    return lax.dot_general(a, b, dims, preferred_element_type=F32)


def smem():
    return pl.BlockSpec(memory_space=pltpu.SMEM)


def whole(array):
    return pl.BlockSpec(array.shape, lambda i: (0,) * array.ndim)


def prep_body(where_ref, gate_ref, up_ref, down_ref, out_ref, gate_t, up_t):
    gate_t[...] = gate_ref[...].T
    up_t[...] = up_ref[...].T
    where = where_ref[0]
    z = where // 2
    core = where % 2
    width = out_ref.shape[3]
    chips = out_ref.shape[1]
    for half in range(2):
        for k in range(chips):
            owner = 2 * ((z + k) % chips) + (core + half) % 2
            rows = pl.ds(pl.multiple_of(owner * width, width), width)
            out_ref[half, k, 0] = gate_t[rows, :]
            out_ref[half, k, 1] = up_t[rows, :]
            out_ref[half, k, 2] = down_ref[rows, :]


def prep(where, w_gate, w_up, w_down, parts):
    width = w_gate.shape[1] // parts
    dim = w_gate.shape[0]
    shape = (2, parts // 2, 3, width, dim)
    return pl.pallas_call(
        prep_body,
        grid=(1,),
        in_specs=[smem(), whole(w_gate), whole(w_up), whole(w_down)],
        out_specs=pl.BlockSpec(shape, lambda i: (0,) * 5),
        out_shape=jax.ShapeDtypeStruct(shape, BF),
        scratch_shapes=[pltpu.VMEM(w_gate.shape[::-1], BF), pltpu.VMEM(w_up.shape[::-1], BF)],
        name="prep",
        compiler_params=pltpu.CompilerParams(vmem_limit_bytes=VMEM_LIMIT),
    )(where, w_gate, w_up, w_down)


def gather_rows(pieces, gu, down):
    k = 0
    rows = down.shape[0]
    for ref in pieces:
        for i in range(ref.shape[0]):
            width = ref.shape[2]
            gu[k * width : (k + 1) * width] = ref[i, 0]
            gu[rows + k * width : rows + (k + 1) * width] = ref[i, 1]
            down[k * width : (k + 1) * width] = ref[i, 2]
            k += 1


def grads_of(x, e, row, gu, down):
    rows = down.shape[0]
    ab = dot(gu[...], x, NT)
    a = ab[:rows]
    b = ab[rows:]
    r = dot(down[...], e, NT) * row
    s = 0.5 + 0.5 * jnp.tanh(0.5 * a)
    act = a * s
    hidden = (act * b * row).astype(BF)
    e_up = (r * act).astype(BF)
    e_gate = (r * b * (s + act * (1.0 - s))).astype(BF)
    return (dot(e_gate, x), dot(e_up, x), dot(hidden, e), hidden)


def mask_row(where, count, step, tile, tokens):
    base = where * tokens + step * tile
    return base + lax.broadcasted_iota(jnp.int32, (1, tile), 1) < count


def half_body(inner, block, n_pieces, has_acc, where_ref, count_ref, scale_ref, rate_ref, x_ref, e_ref, *refs):
    pieces = refs[:n_pieces]
    refs = refs[n_pieces:]
    if has_acc:
        start_ref = refs[0]
        refs = refs[1:]
    out_ref, gu, down, acc = refs
    step = pl.program_id(0)
    tile = x_ref.shape[2]
    tokens = tile * pl.num_programs(0)

    @pl.when(step == 0)
    def _():
        gather_rows(pieces, gu, down)

    count = count_ref[0, block]
    valid = mask_row(where_ref[0], count, step, tile, tokens)
    if inner:
        factor = -(scale_ref[0] / count.astype(F32))
        row = jnp.where(valid, rate_ref[0, block : block + 1, :] * factor, 0.0)
    else:
        row = jnp.where(valid, 1.0, 0.0)
    g, u, d, _ = grads_of(x_ref[0, 0], e_ref[0, 0], row, gu, down)
    g = (g, u, d)

    @pl.when(step == 0)
    def _():
        for j in range(3):
            acc[j] = (start_ref[j] + g[j]) if has_acc else g[j]

    @pl.when(step != 0)
    def _():
        for j in range(3):
            acc[j] += g[j]

    @pl.when(step == pl.num_programs(0) - 1)
    def _():
        out_ref[...] = acc[...].astype(out_ref.dtype)


def half_grads(inner, block, where, count, scale, rate, x, e, pieces, out_dtype, acc=None, tile=512):
    tokens, dim = x.shape[2:]
    n_rows = sum(p.shape[0] * p.shape[2] for p in pieces)
    shape = (3, n_rows, dim)
    steps = tokens // tile
    operands = [where, count, scale, rate, x, e, *pieces]
    spec = pl.BlockSpec((1, 1, tile, dim), lambda i: (0, block, i, 0))
    specs = [smem(), smem(), smem(), pl.BlockSpec((1, rate.shape[1], tile), lambda i: (0, 0, i)), spec, spec]
    specs += [whole(p) for p in pieces]
    if acc is not None:
        operands.append(acc)
        specs.append(whole(acc))
    return pl.pallas_call(
        functools.partial(half_body, inner, block, len(pieces), acc is not None),
        grid=(steps,),
        in_specs=specs,
        out_specs=pl.BlockSpec(shape, lambda i: (0, 0, 0)),
        out_shape=jax.ShapeDtypeStruct(shape, out_dtype),
        scratch_shapes=[
            pltpu.VMEM((2 * n_rows, dim), BF),
            pltpu.VMEM((n_rows, dim), BF),
            pltpu.VMEM(shape, F32),
        ],
        name=("inner" if inner else "outer") + str(block),
        cost_estimate=pl.CostEstimate(
            flops=12 * tokens * n_rows * dim, transcendentals=tokens * n_rows, bytes_accessed=4 * tokens * dim
        ),
        compiler_params=pltpu.CompilerParams(vmem_limit_bytes=VMEM_LIMIT),
    )(*operands)


def output_body(block, n_pieces, where_ref, count_ref, x_ref, *refs):
    pieces = refs[:n_pieces]
    out_ref, gu, down = refs[-3:]
    step = pl.program_id(0)
    tile = x_ref.shape[2]

    @pl.when(step == 0)
    def _():
        gather_rows(pieces, gu, down)

    valid = mask_row(where_ref[0], count_ref[0, block], step, tile, tile * pl.num_programs(0))
    rows = down.shape[0]
    ab = dot(gu[...], x_ref[0, 0], NT)
    a = ab[:rows]
    s = 0.5 + 0.5 * jnp.tanh(0.5 * a)
    hidden = jnp.where(valid, a * s * ab[rows:], 0.0).astype(BF)
    out_ref[0, 0] = dot(hidden, down[...], TN).astype(BF)


def output_of(block, where, count, x, pieces, base=None, tile=512):
    tokens, dim = x.shape[2:]
    n_rows = sum(p.shape[0] * p.shape[2] for p in pieces)
    spec = pl.BlockSpec((1, 1, tile, dim), lambda i: (0, block, i, 0))
    operands = [where, count, x, *pieces]
    specs = [smem(), smem(), spec] + [whole(p) for p in pieces]
    alias = {}
    if base is not None:
        alias = {len(operands): 0}
        operands.append(base)
        specs.append(pl.BlockSpec(memory_space=pl.ANY))
    return pl.pallas_call(
        functools.partial(output_body, block, len(pieces)),
        grid=(tokens // tile,),
        in_specs=specs,
        out_specs=spec,
        out_shape=jax.ShapeDtypeStruct(x.shape, BF),
        scratch_shapes=[pltpu.VMEM((2 * n_rows, dim), BF), pltpu.VMEM((n_rows, dim), BF)],
        input_output_aliases=alias,
        name="output" + str(block),
        cost_estimate=pl.CostEstimate(
            flops=6 * tokens * n_rows * dim, transcendentals=tokens * n_rows, bytes_accessed=4 * tokens * dim
        ),
        compiler_params=pltpu.CompilerParams(vmem_limit_bytes=VMEM_LIMIT),
    )(*operands)


def combine_body(own_ref, other_ref, *outs):
    width = outs[0].shape[1]
    for k, out in enumerate(outs):
        rows = slice(k * width, (k + 1) * width)
        out[...] = (own_ref[:, rows, :].astype(F32) + other_ref[:, rows, :].astype(F32)).astype(out.dtype)


def combine(own, other, chips):
    shape = (3, own.shape[1] // chips, own.shape[2])
    spec = pl.BlockSpec(shape, lambda i: (0, 0, 0))
    return pl.pallas_call(
        combine_body,
        grid=(1,),
        in_specs=[whole(own), whole(other)],
        out_specs=[spec] * chips,
        out_shape=[jax.ShapeDtypeStruct(shape, F32 if k == 0 else BF) for k in range(chips)],
        name="combine",
        compiler_params=pltpu.CompilerParams(vmem_limit_bytes=VMEM_LIMIT),
    )(own, other)


def norm_of(w):
    return jnp.sqrt(jnp.sum(w * w, axis=1, keepdims=True) + TINY)


def update_body(first, n_recv, scale_ref, own_ref, *refs):
    recv = refs[:n_recv]
    refs = refs[n_recv:]
    if first:
        start_ref, piece_ref, level_ref, state_out, momentum_out, norm_out = refs
    else:
        state_ref, momentum_ref, norm_ref, piece_ref, level_ref = refs
    scale = scale_ref[0]
    for j in range(3):
        total = own_ref[j]
        for ref in recv:
            total = total + ref[j].astype(F32)
        if j == 0:
            level = jnp.max(jnp.abs(total), axis=1, keepdims=True)
            level_ref[...] = jnp.broadcast_to(level, level_ref.shape)
        if first:
            state = start_ref[0, 0, j].astype(F32)
            norm = norm_of(state)
            moved = total / scale
        else:
            state = state_ref[j]
            norm = norm_ref[j][:, :1]
            moved = KEEP * momentum_ref[j] + total / scale
        state = state - RATE * moved
        state = state * (norm / norm_of(state))
        piece_ref[0, j] = state.astype(BF)
        if first:
            state_out[j] = state
            momentum_out[j] = moved
            norm_out[j] = jnp.broadcast_to(norm, norm_out.shape[1:])


def update(scale, own, recv, start=None, carried=None):
    first = start is not None
    operands = [scale, own, *recv]
    specs = [smem(), whole(own)] + [whole(r) for r in recv]
    if first:
        operands.append(start)
        specs.append(pl.BlockSpec((1, 1) + start.shape[2:], lambda i: (0,) * 5))
    else:
        operands += list(carried)
        specs += [whole(c) for c in carried]
    shapes = [((1,) + own.shape, BF), ((own.shape[1], 128), F32)]
    if first:
        shapes += [(own.shape, F32), (own.shape, F32), (own.shape[:2] + (128,), F32)]
    return pl.pallas_call(
        functools.partial(update_body, first, len(recv)),
        grid=(1,),
        in_specs=specs,
        out_specs=[pl.BlockSpec(s, lambda i, n=len(s): (0,) * n) for s, _ in shapes],
        out_shape=[jax.ShapeDtypeStruct(s, t) for s, t in shapes],
        name="update",
        compiler_params=pltpu.CompilerParams(vmem_limit_bytes=VMEM_LIMIT),
    )(*operands)


def per_device(
    keys, values, queries, token_rate, valid_count, loss_scale, w_gate, w_up, w_down, out_cotangent
):
    parts = lax.axis_size("tok")
    seqs = lax.axis_size("seq")
    chips = parts // 2
    where = lax.axis_index("tok").reshape(1).astype(jnp.int32)

    def z_shift(array, k):
        pairs = [(2 * z + c, 2 * ((z + k) % chips) + c) for z in range(chips) for c in range(2)]
        return lax.ppermute(array, "tok", pairs)

    def other_core(array):
        return lax.ppermute(array, "tok", [(t, t ^ 1) for t in range(parts)])

    def scatter(own, other):
        sums = combine(own, other_core(other), chips)
        return sums[0], [z_shift(sums[k], k) for k in range(1, chips)]

    def spread(piece):
        mine = [piece] + [z_shift(piece, chips - k) for k in range(1, chips)]
        return mine, [other_core(p) for p in mine]

    start = prep(where, w_gate, w_up, w_down, parts)
    halves = ([start[0]], [start[1]])
    args = (where, valid_count, loss_scale, token_rate)
    levels = []
    carried = None
    for block in range(2):
        other = half_grads(True, block, *args, keys, values, halves[1], BF)
        own = half_grads(True, block, *args, keys, values, halves[0], F32)
        own, recv = scatter(own, other)
        if block == 0:
            piece, level, *carried = update(loss_scale, own, recv, start=start)
        else:
            piece, level = update(loss_scale, own, recv, carried=carried)
        levels.append(level[:, 0])
        halves = spread(piece)
        if block == 0:
            acc = [
                half_grads(False, 0, *args, queries, out_cotangent, halves[h], F32) for h in range(2)
            ]
            fast_out = output_of(0, where, valid_count, queries, halves[0] + halves[1])
    other = half_grads(False, 1, *args, queries, out_cotangent, halves[1], BF, acc=acc[1])
    own = half_grads(False, 1, *args, queries, out_cotangent, halves[0], F32, acc=acc[0])
    fast_out = output_of(1, where, valid_count, queries, halves[0] + halves[1], base=fast_out)
    own, recv = scatter(own, other)
    total = own
    for r in recv:
        total = total + r.astype(F32)
    shape = total.shape
    rows = shape[0] * shape[1] // seqs
    total = total.astype(BF).reshape(seqs, rows, shape[2])
    total = lax.all_to_all(total, "seq", 0, 0)
    total = jnp.sum(total.astype(F32), axis=0).astype(BF)
    level = jnp.concatenate(levels)
    high = lax.reduce_precision(level, 8, 7)
    mid = lax.reduce_precision(level - high, 8, 7)
    low = level - high - mid
    line = jnp.concatenate([high.astype(BF), mid.astype(BF), low.astype(BF), jnp.zeros((shape[2] - 3 * level.shape[0],), BF)])
    sent = jnp.concatenate([total, line[None]])
    sent = jnp.broadcast_to(sent[None], (seqs,) + sent.shape)
    got = lax.all_to_all(sent, "seq", 0, 0).astype(F32)
    total = got[:, :rows].reshape(shape)
    size = level.shape[0]
    line = got[:, rows]
    level = line[:, :size] + line[:, size : 2 * size] + line[:, 2 * size : 3 * size]
    level = jnp.max(level, axis=0).reshape(2, shape[1])
    return (fast_out, total[0].T, total[1].T, total[2], level)


def solution(mesh):
    placed = (
        P("seq", None, "tok", None),
        P("seq", None, "tok", None),
        P("seq", None, "tok", None),
        P("seq", None, "tok"),
        P("seq", None),
        P(),
        P(),
        P(),
        P(),
        P("seq", None, "tok", None),
    )
    return jax.shard_map(
        per_device,
        mesh=mesh,
        in_specs=placed,
        out_specs=(
            P("seq", None, "tok", None),
            P(None, "tok"),
            P(None, "tok"),
            P("tok", None),
            P(None, "tok"),
        ),
        check_vma=False,
    )
```

```python
import functools
import jax
import jax.numpy as jnp
from jax import lax
from jax.experimental import pallas as pl
from jax.experimental.pallas import tpu as pltpu
from jax.sharding import PartitionSpec as P


KEEP = 0.9
RATE = 3.0
TINY = 1e-06
BF = jnp.bfloat16
F32 = jnp.float32
NT = (((1,), (1,)), ((), ()))
TN = (((0,), (0,)), ((), ()))
MIB = 1024 * 1024
TILE = 512


def dot(a, b, dims=None):
    if dims is None:
        return jnp.dot(a, b, preferred_element_type=F32)
    return lax.dot_general(a, b, dims, preferred_element_type=F32)


VMEM = pl.BlockSpec(memory_space=pltpu.VMEM)
SMEM = pl.BlockSpec(memory_space=pltpu.SMEM)


def call(body, operands, n_smem, outs, scratch=(), limit=8, flops=0, n_exp=0):
    shapes = [jax.ShapeDtypeStruct(s, t) for s, t in outs]
    cost = None
    if flops:
        cost = pl.CostEstimate(flops=flops, transcendentals=n_exp, bytes_accessed=4 * MIB)
    return pl.pallas_call(
        body,
        in_specs=[SMEM] * n_smem + [VMEM] * (len(operands) - n_smem),
        out_specs=[VMEM] * len(shapes),
        out_shape=shapes,
        scratch_shapes=list(scratch),
        cost_estimate=cost,
        compiler_params=pltpu.CompilerParams(vmem_limit_bytes=limit * MIB),
    )(*operands)


def prep_body(where_ref, gate_ref, up_ref, down_ref, *refs):
    outs = refs[:2]
    gate_t, up_t = refs[2:]
    gate_t[...] = gate_ref[...].T
    up_t[...] = up_ref[...].T
    where = where_ref[0]
    z = where // 2
    core = where % 2
    chips, _, width, _ = outs[0].shape
    for half in range(2):
        for k in range(chips):
            owner = 2 * ((z + k) % chips) + (core + half) % 2
            rows = pl.ds(pl.multiple_of(owner * width, width), width)
            outs[half][k, 0] = gate_t[rows, :]
            outs[half][k, 1] = up_t[rows, :]
            outs[half][k, 2] = down_ref[rows, :]


def prep(where, w_gate, w_up, w_down, parts):
    dim, hid = w_gate.shape
    shape = (parts // 2, 3, hid // parts, dim)
    return call(
        prep_body,
        (where, w_gate, w_up, w_down),
        1,
        [(shape, BF)] * 2,
        scratch=[pltpu.VMEM((hid, dim), BF)] * 2,
    )


def gather_rows(pieces, gu, down):
    k = 0
    rows = down.shape[0]
    for ref in pieces:
        n, _, width, _ = ref.shape
        for i in range(n):
            gu[k * width : (k + 1) * width] = ref[i, 0]
            gu[rows + k * width : rows + (k + 1) * width] = ref[i, 1]
            down[k * width : (k + 1) * width] = ref[i, 2]
            k += 1


def mask_row(where, count, start, size, tokens):
    base = where * tokens + start
    return base + lax.broadcasted_iota(jnp.int32, (1, size), 1) < count


def grads_body(inner, block, n_pieces, skip, result, where_ref, count_ref, scale_ref, rate_ref, x_ref, e_ref, *refs):
    pieces = refs[:n_pieces]
    refs = refs[n_pieces:]
    has_acc = skip is not None
    if has_acc:
        start_ref = refs[0]
        refs = refs[1:]
    if result:
        out_ref, result_ref, gu, down, acc = refs
    else:
        out_ref, gu, down, acc = refs
    gather_rows(pieces, gu, down)
    rows = down.shape[0]
    tokens = x_ref.shape[2]
    count = count_ref[0, block]
    steps = tokens // TILE
    for i in range(steps):
        span = slice(i * TILE, (i + 1) * TILE)
        x = x_ref[0, block, span]
        e = e_ref[0, block, span]
        valid = mask_row(where_ref[0], count, i * TILE, TILE, tokens)
        if inner:
            factor = -(scale_ref[0] / count.astype(F32))
            row = jnp.where(valid, rate_ref[0, block : block + 1, span] * factor, 0.0)
        else:
            row = jnp.where(valid, 1.0, 0.0)
        ab = dot(gu[...], x, NT)
        a = ab[:rows]
        b = ab[rows:]
        r = dot(down[...], e, NT) * row
        s = 0.5 + 0.5 * jnp.tanh(0.5 * a)
        act = a * s
        hidden = (act * b * row).astype(BF)
        e_up = (r * act).astype(BF)
        e_gate = (r * b * (s + act * (1.0 - s))).astype(BF)
        for j, (left, right) in enumerate(((e_gate, x), (e_up, x), (hidden, e))):
            value = dot(left, right)
            if i > 0:
                value = value + acc[j]
            elif has_acc:
                value = value + start_ref[j, skip : skip + rows]
            if i == steps - 1:
                out_ref[j] = value.astype(out_ref.dtype)
            else:
                acc[j] = value
        if result:
            result_ref[span] = dot(hidden, down[...], TN).astype(BF)


def grads(inner, block, args, x, e, pieces, out_dtype, acc=None, skip=None, result=False):
    tokens, dim = x.shape[2:]
    n_rows = sum(p.shape[0] * p.shape[2] for p in pieces)
    shape = (3, n_rows, dim)
    operands = [*args, x, e, *pieces]
    if acc is not None:
        operands.append(acc)
    outs = [(shape, out_dtype)]
    if result:
        outs.append(((tokens, dim), BF))
    return call(
        functools.partial(grads_body, inner, block, len(pieces), skip, result),
        operands,
        3,
        outs,
        scratch=[pltpu.VMEM((2 * n_rows, dim), BF), pltpu.VMEM((n_rows, dim), BF), pltpu.VMEM(shape, F32)],
        limit=20,
        flops=12 * tokens * n_rows * dim,
        n_exp=tokens * n_rows,
    )


def output_body(block, n_pieces, where_ref, count_ref, x_ref, done_ref, *refs):
    out_ref, gu, down = refs[-3:]
    gather_rows(refs[:n_pieces], gu, down)
    rows = down.shape[0]
    tokens = x_ref.shape[2]
    for other in range(block):
        out_ref[0, other] = done_ref[...]
    for i in range(tokens // TILE):
        span = slice(i * TILE, (i + 1) * TILE)
        valid = mask_row(where_ref[0], count_ref[0, block], i * TILE, TILE, tokens)
        ab = dot(gu[...], x_ref[0, block, span], NT)
        a = ab[:rows]
        s = 0.5 + 0.5 * jnp.tanh(0.5 * a)
        hidden = jnp.where(valid, a * s * ab[rows:], 0.0).astype(BF)
        out_ref[0, block, span] = dot(hidden, down[...], TN).astype(BF)


def output_of(where, count, x, done, pieces):
    tokens, dim = x.shape[2:]
    n_rows = sum(p.shape[0] * p.shape[2] for p in pieces)
    return call(
        functools.partial(output_body, 1, len(pieces)),
        [where, count, x, done, *pieces],
        2,
        [(x.shape, BF)],
        scratch=[pltpu.VMEM((2 * n_rows, dim), BF), pltpu.VMEM((n_rows, dim), BF)],
        limit=16,
        flops=6 * tokens * n_rows * dim,
        n_exp=tokens * n_rows,
    )[0]


def combine_body(own_ref, other_ref, *outs):
    width = outs[0].shape[1]
    for k, out in enumerate(outs):
        rows = slice(k * width, (k + 1) * width)
        out[...] = (own_ref[:, rows, :].astype(F32) + other_ref[:, rows, :].astype(F32)).astype(out.dtype)


def combine(own, other, chips):
    shape = (3, own.shape[1] // chips, own.shape[2])
    outs = [(shape, F32 if k == 0 else BF) for k in range(chips)]
    return call(combine_body, (own, other), 0, outs)


def norm_of(w):
    return jnp.sqrt(jnp.sum(w * w, axis=1, keepdims=True) + TINY)


def update_body(first, n_recv, scale_ref, own_ref, *refs):
    recv = refs[:n_recv]
    refs = refs[n_recv:]
    if first:
        start_ref, piece_ref, level_ref, state_out, momentum_out, norm_out = refs
    else:
        state_ref, momentum_ref, norm_ref, piece_ref, level_ref = refs
    scale = scale_ref[0]
    for j in range(3):
        total = own_ref[j]
        for ref in recv:
            total = total + ref[j].astype(F32)
        if j == 0:
            level = jnp.max(jnp.abs(total), axis=1, keepdims=True)
            level = jnp.broadcast_to(level, (level.shape[0], 128)).T
            level_ref[...] = level[: level_ref.shape[0]]
        if first:
            state = start_ref[0, j].astype(F32)
            norm = norm_of(state)
            moved = total / scale
        else:
            state = state_ref[j]
            norm = norm_ref[j][:, :1]
            moved = KEEP * momentum_ref[j] + total / scale
        state = state - RATE * moved
        state = state * (norm / norm_of(state))
        piece_ref[0, j] = state.astype(BF)
        if first:
            state_out[j] = state
            momentum_out[j] = moved
            norm_out[j] = jnp.broadcast_to(norm, norm_out.shape[1:])


def update(scale, own, recv, start=None, carried=None):
    first = start is not None
    operands = [scale, own, *recv] + ([start] if first else list(carried))
    outs = [((1,) + own.shape, BF), ((8, own.shape[1]), F32)]
    if first:
        outs += [(own.shape, F32), (own.shape, F32), (own.shape[:2] + (128,), F32)]
    return call(functools.partial(update_body, first, len(recv)), operands, 1, outs)


def cells(rows, dim, seqs):
    across = seqs * 8 // rows
    return [(8 * (s // across), (s % across) * (dim // across)) for s in range(seqs)], dim // across


def deal_body(seqs, own_ref, *refs):
    out_ref = refs[-1]
    n, rows, dim = own_ref.shape
    spots, lanes = cells(rows, dim, seqs)
    for j in range(n):
        total = own_ref[j]
        for ref in refs[:-1]:
            total = total + ref[j].astype(F32)
        total = total.astype(BF)
        for s, (row, lane) in enumerate(spots):
            out_ref[s, j] = total[row : row + 8, lane : lane + lanes]


def deal(own, recv, seqs):
    n, rows, dim = own.shape
    shape = (seqs, n, 8, cells(rows, dim, seqs)[1])
    return call(functools.partial(deal_body, seqs), (own, *recv), 0, [(shape, BF)])[0]


def fold_body(got_ref, first_ref, second_ref, out_ref):
    seqs, n = got_ref.shape[:2]
    width = first_ref.shape[1]
    values = []
    for j in range(n):
        total = got_ref[0, j].astype(F32)
        for s in range(1, seqs):
            total = total + got_ref[s, j].astype(F32)
        values.append(total.astype(BF))
    level = jnp.zeros(got_ref.shape[2:], F32)
    pad = jnp.zeros((8, 128 - width), F32)
    level = jnp.concatenate([first_ref[...], pad, second_ref[...], pad], axis=1)
    high = level.astype(BF).astype(F32)
    mid = (level - high).astype(BF).astype(F32)
    low = level - high - mid
    line = lax.broadcasted_iota(jnp.int32, level.shape, 0)
    level = jnp.where(line == 0, high, jnp.where(line == 1, mid, low))
    values.append(level.astype(BF))
    for s in range(seqs):
        for j in range(n + 1):
            out_ref[s, j] = values[j]


def fold(got, first, second):
    seqs, n, rows, lanes = got.shape
    return call(fold_body, (got, first, second), 0, [((seqs, n + 1, rows, lanes), BF)])[0]


def finish_body(got_ref, gate_ref, up_ref, down_ref, level_ref):
    seqs, n = got_ref.shape[:2]
    rows, dim = down_ref.shape
    spots, lanes = cells(rows, dim, seqs)
    for j in range(n - 1):
        target = (gate_ref, up_ref, down_ref)[j]
        for s, (row, lane) in enumerate(spots):
            target[row : row + 8, lane : lane + lanes] = got_ref[s, j].astype(F32)
    best = None
    for s in range(seqs):
        terms = got_ref[s, n - 1].astype(F32)
        value = terms[0:1] + terms[1:2] + terms[2:3]
        best = value if best is None else jnp.maximum(best, value)
    level_ref[0:1, :] = best[:, :rows]
    level_ref[1:2, :] = best[:, 128 : 128 + rows]


def finish(got, rows, dim):
    outs = [((rows, dim), F32)] * 3 + [((2, rows), F32)]
    return call(finish_body, (got,), 0, outs)


def per_device(
    keys, values, queries, token_rate, valid_count, loss_scale, w_gate, w_up, w_down, out_cotangent
):
    parts = lax.axis_size("tok")
    seqs = lax.axis_size("seq")
    chips = parts // 2
    where = lax.axis_index("tok").reshape(1).astype(jnp.int32)

    def z_shift(array, k):
        pairs = [(2 * z + c, 2 * ((z + k) % chips) + c) for z in range(chips) for c in range(2)]
        return lax.ppermute(array, "tok", pairs)

    def other_core(array):
        return lax.ppermute(array, "tok", [(t, t ^ 1) for t in range(parts)])

    def scatter(own, other):
        sums = combine(own, other_core(other), chips)
        recv = []
        for k in range(1, chips):
            recv.append(z_shift(sums[k], k))
        return sums[0], recv

    def spread(piece):
        mine = [piece] + [z_shift(piece, chips - k) for k in range(1, chips)]
        return mine, [other_core(p) for p in mine]

    first, second = prep(where, w_gate, w_up, w_down, parts)
    half = w_gate.shape[1] // 2
    args = (where, valid_count, loss_scale, token_rate)

    def inner(block, halves):
        other = grads(True, block, args, keys, values, halves[1], BF)[0]
        own = grads(True, block, args, keys, values, halves[0], F32)[0]
        return scatter(own, other)

    own, recv = inner(0, ([first], [second]))
    piece, level0, *carried = update(loss_scale, own, recv, start=first)
    halves = spread(piece)
    acc, done = grads(False, 0, args, queries, out_cotangent, halves[0] + halves[1], F32, result=True)
    own, recv = inner(1, halves)
    piece, level1 = update(loss_scale, own, recv, carried=carried)
    halves = spread(piece)
    other = grads(False, 1, args, queries, out_cotangent, halves[1], BF, acc=acc, skip=half)[0]
    own = grads(False, 1, args, queries, out_cotangent, halves[0], F32, acc=acc, skip=0)[0]
    own, recv = scatter(own, other)
    fast_out = output_of(where, valid_count, queries, done, halves[0] + halves[1])
    dealt = lax.all_to_all(deal(own, recv, seqs), "seq", 0, 0)
    got = lax.all_to_all(fold(dealt, level0, level1), "seq", 0, 0)
    gate, up, down, level = finish(got, own.shape[1], own.shape[2])
    return (fast_out, gate.T, up.T, down, level)


def solution(mesh):
    placed = (
        P("seq", None, "tok", None),
        P("seq", None, "tok", None),
        P("seq", None, "tok", None),
        P("seq", None, "tok"),
        P("seq", None),
        P(),
        P(),
        P(),
        P(),
        P("seq", None, "tok", None),
    )

    return jax.shard_map(
        per_device,
        mesh=mesh,
        in_specs=placed,
        out_specs=(
            P("seq", None, "tok", None),
            P(None, "tok"),
            P(None, "tok"),
            P("tok", None),
            P(None, "tok"),
        ),
        check_vma=False,
    )
```

```python
import functools
import math
import jax
import jax.numpy as jnp
from jax import lax
from jax.experimental import pallas as pl
from jax.experimental.pallas import tpu as pltpu
from jax.sharding import PartitionSpec as P


KEEP = 0.9
RATE = 3.0
TINY = 1e-06
BF = jnp.bfloat16
F32 = jnp.float32
NT = (((1,), (1,)), ((), ()))
TN = (((0,), (0,)), ((), ()))
MIB = 1024 * 1024
TILE = 512


def dot(a, b, dims=None):
    if dims is None:
        return jnp.dot(a, b, preferred_element_type=F32)
    return lax.dot_general(a, b, dims, preferred_element_type=F32)


VMEM = pl.BlockSpec(memory_space=pltpu.VMEM)
SMEM = pl.BlockSpec(memory_space=pltpu.SMEM)
ANY = pl.BlockSpec(memory_space=pltpu.HBM)


def call(body, operands, n_smem, outs, scratch=(), limit=8, flops=0, n_exp=0, n_any=0):
    shapes = [jax.ShapeDtypeStruct(s, t) for s, t in outs]
    cost = None
    if flops:
        cost = pl.CostEstimate(flops=flops, transcendentals=n_exp, bytes_accessed=4 * MIB)
    return pl.pallas_call(
        body,
        in_specs=[ANY] * n_any + [SMEM] * n_smem + [VMEM] * (len(operands) - n_smem - n_any),
        out_specs=[VMEM] * len(shapes),
        out_shape=shapes,
        scratch_shapes=list(scratch),
        cost_estimate=cost,
        compiler_params=pltpu.CompilerParams(vmem_limit_bytes=limit * MIB),
    )(*operands)


def gather_rows(pieces, gu, down):
    k = 0
    rows = down.shape[0]
    for ref in pieces:
        n, _, width, _ = ref.shape
        for i in range(n):
            gu[k * width : (k + 1) * width] = ref[i, 0]
            gu[rows + k * width : rows + (k + 1) * width] = ref[i, 1]
            down[k * width : (k + 1) * width] = ref[i, 2]
            k += 1


def mask_row(count, start, size, tokens):
    base = lax.axis_index("tok") * tokens + start
    return base + lax.broadcasted_iota(jnp.int32, (1, size), 1) < count


def inner_row(count, scale, rate, start, tokens):
    size = rate.shape[1]
    return jnp.where(mask_row(count, start, size, tokens), rate * -(scale / count.astype(F32)), 0.0)


def outer_row(count, start, size, tokens):
    return jnp.where(mask_row(count, start, size, tokens), 1.0, 0.0)


def tile_grads(x, e, row, gu, down):
    rows = down.shape[0]
    ab = dot(gu[...], x, NT)
    a = ab[:rows]
    b = ab[rows:]
    r = dot(down[...], e, NT) * row
    s = 0.5 + 0.5 * jnp.tanh(0.5 * a)
    act = a * s
    hidden = (act * b * row).astype(BF)
    e_up = (r * act).astype(BF)
    e_gate = (r * b * (s + act * (1.0 - s))).astype(BF)
    return ((e_gate, x), (e_up, x), (hidden, e))


def add_grads(pairs, i, steps, acc, out_ref, start=None):
    for j, (left, right) in enumerate(pairs):
        value = dot(left, right)
        if i > 0:
            value = value + acc[j]
        elif start is not None:
            value = value + start(j)
        if i == steps - 1:
            out_ref[j] = value.astype(out_ref.dtype)
        else:
            acc[j] = value


def grad_scratch(n_rows, dim):
    return [pltpu.VMEM((2 * n_rows, dim), BF), pltpu.VMEM((n_rows, dim), BF), pltpu.VMEM((3, n_rows, dim), F32)]


def grad_cost(tokens, n_rows, dim):
    return dict(limit=20, flops=12 * tokens * n_rows * dim, n_exp=tokens * n_rows)


def lead_body(keys_ref, values_ref, rate_hbm, gate_hbm, up_hbm, down_hbm, count_hbm, scale_ref, *refs):
    out_ref, x_ref, e_ref, first_ref, second_ref = refs[:5]
    gate_ref, up_ref, down_ref, gate_t, up_t, rate_ref, count_ref, gu, down, acc, sems = refs[5:]
    tokens = x_ref.shape[0]
    steps = tokens // TILE
    spans = [slice(i * TILE, (i + 1) * TILE) for i in range(steps)]
    copies = [(gate_hbm, gate_ref), (up_hbm, up_ref), (down_hbm, down_ref)]
    copies += [(count_hbm, count_ref), (rate_hbm, rate_ref)]
    for span in spans:
        copies += [(keys_ref.at[0, 0, span], x_ref.at[span]), (values_ref.at[0, 0, span], e_ref.at[span])]
    copies = [pltpu.make_async_copy(a, b, sems.at[n]) for n, (a, b) in enumerate(copies)]
    for copy in copies:
        copy.start()
    where = lax.axis_index("tok")
    z = where // 2
    core = where % 2
    chips, _, width, _ = first_ref.shape
    copies[0].wait()
    gate_t[...] = gate_ref[...].T
    copies[1].wait()
    up_t[...] = up_ref[...].T
    copies[2].wait()
    for half, out in enumerate((first_ref, second_ref)):
        for k in range(chips):
            owner = 2 * ((z + k) % chips) + (core + half) % 2
            rows = pl.ds(pl.multiple_of(owner * width, width), width)
            out[k, 0] = gate_t[rows, :]
            out[k, 1] = up_t[rows, :]
            out[k, 2] = down_ref[rows, :]
    gather_rows((second_ref,), gu, down)
    for n in range(3, 5):
        copies[n].wait()
    for i, span in enumerate(spans):
        copies[5 + 2 * i].wait()
        copies[6 + 2 * i].wait()
        row = inner_row(count_ref[0, 0], scale_ref[0], rate_ref[0, 0:1, span], i * TILE, tokens)
        pairs = tile_grads(x_ref[span], e_ref[span], row, gu, down)
        add_grads(pairs, i, steps, acc, out_ref)


def lead(keys, values, rate, w_gate, w_up, w_down, count, scale, parts):
    tokens, dim = keys.shape[2:]
    hid = w_gate.shape[1]
    half = hid // 2
    piece = (parts // 2, 3, hid // parts, dim)
    outs = [((3, half, dim), BF), ((tokens, dim), BF), ((tokens, dim), BF), (piece, BF), (piece, BF)]
    scratch = [pltpu.VMEM(w.shape, BF) for w in (w_gate, w_up, w_down)]
    scratch += [pltpu.VMEM((hid, dim), BF)] * 2
    scratch += [pltpu.VMEM(rate.shape, F32), pltpu.SMEM(count.shape, jnp.int32)]
    scratch += grad_scratch(half, dim) + [pltpu.SemaphoreType.DMA((5 + 2 * (tokens // TILE),))]
    operands = (keys, values, rate, w_gate, w_up, w_down, count)
    operands = [pltpu.with_memory_space_constraint(array, pltpu.HBM) for array in operands] + [scale]
    return call(lead_body, operands, 1, outs, scratch, n_any=7, **grad_cost(tokens, half, dim))


def grads_body(inner, block, n_pieces, skip, result, count_ref, scale_ref, rate_ref, x_ref, e_ref, *refs):
    pieces = refs[:n_pieces]
    refs = refs[n_pieces:]
    start = None
    if skip is not None:
        start_ref = refs[0]
        refs = refs[1:]
    out_ref, gu, down, acc = refs[0], *refs[-3:]
    gather_rows(pieces, gu, down)
    rows = down.shape[0]
    if skip is not None:
        start = lambda j: start_ref[j, skip : skip + rows]
    flat = len(x_ref.shape) == 2
    tokens = x_ref.shape[-2]
    count = count_ref[0, block]
    steps = tokens // TILE
    for i in range(steps):
        span = slice(i * TILE, (i + 1) * TILE)
        x = x_ref[span] if flat else x_ref[0, block, span]
        e = e_ref[span] if flat else e_ref[0, block, span]
        if inner:
            row = inner_row(count, scale_ref[0], rate_ref[0, block : block + 1, span], i * TILE, tokens)
        else:
            row = outer_row(count, i * TILE, TILE, tokens)
        pairs = tile_grads(x, e, row, gu, down)
        add_grads(pairs, i, steps, acc, out_ref, start)
        if result:
            refs[1][span] = dot(pairs[2][0], down[...], TN).astype(BF)


def grads(inner, block, args, x, e, pieces, out_dtype, acc=None, skip=None, result=False):
    tokens, dim = x.shape[-2:]
    n_rows = sum(p.shape[0] * p.shape[2] for p in pieces)
    operands = [*args, x, e, *pieces]
    if acc is not None:
        operands.append(acc)
    outs = [((3, n_rows, dim), out_dtype)]
    if result:
        outs.append(((tokens, dim), BF))
    return call(
        functools.partial(grads_body, inner, block, len(pieces), skip, result),
        operands,
        2,
        outs,
        grad_scratch(n_rows, dim),
        **grad_cost(tokens, n_rows, dim),
    )


def output_body(block, n_pieces, count_ref, x_ref, done_ref, *refs):
    out_ref, gu, down = refs[-3:]
    gather_rows(refs[:n_pieces], gu, down)
    rows = down.shape[0]
    tokens = x_ref.shape[2]
    for other in range(block):
        out_ref[0, other] = done_ref[...]
    for i in range(tokens // TILE):
        span = slice(i * TILE, (i + 1) * TILE)
        valid = mask_row(count_ref[0, block], i * TILE, TILE, tokens)
        ab = dot(gu[...], x_ref[0, block, span], NT)
        a = ab[:rows]
        s = 0.5 + 0.5 * jnp.tanh(0.5 * a)
        hidden = jnp.where(valid, a * s * ab[rows:], 0.0).astype(BF)
        out_ref[0, block, span] = dot(hidden, down[...], TN).astype(BF)


def output_of(count, x, done, pieces):
    tokens, dim = x.shape[2:]
    n_rows = sum(p.shape[0] * p.shape[2] for p in pieces)
    return call(
        functools.partial(output_body, 1, len(pieces)),
        [count, x, done, *pieces],
        1,
        [(x.shape, BF)],
        scratch=[pltpu.VMEM((2 * n_rows, dim), BF), pltpu.VMEM((n_rows, dim), BF)],
        limit=16,
        flops=6 * tokens * n_rows * dim,
        n_exp=tokens * n_rows,
    )[0]


def combine_body(own_ref, other_ref, *outs):
    width = outs[0].shape[1]
    for k, out in enumerate(outs):
        rows = slice(k * width, (k + 1) * width)
        out[...] = (own_ref[:, rows, :].astype(F32) + other_ref[:, rows, :].astype(F32)).astype(out.dtype)


def combine(own, other, chips):
    shape = (3, own.shape[1] // chips, own.shape[2])
    outs = [(shape, F32 if k == 0 else BF) for k in range(chips)]
    return call(combine_body, (own, other), 0, outs)


def norm_of(w):
    return jnp.sqrt(jnp.sum(w * w, axis=1, keepdims=True) + TINY)


def update_body(first, n_recv, scale_ref, own_ref, *refs):
    recv = refs[:n_recv]
    refs = refs[n_recv:]
    if first:
        start_ref, piece_ref, level_ref, state_out, momentum_out, norm_out = refs
    else:
        state_ref, momentum_ref, norm_ref, piece_ref, level_ref = refs
    scale = scale_ref[0]
    for j in range(3):
        total = own_ref[j]
        for ref in recv:
            total = total + ref[j].astype(F32)
        if j == 0:
            level = jnp.max(jnp.abs(total), axis=1, keepdims=True)
            level = jnp.broadcast_to(level, (level.shape[0], 128)).T
            level_ref[...] = level[: level_ref.shape[0]]
        if first:
            state = start_ref[0, j].astype(F32)
            norm = norm_of(state)
            moved = total / scale
        else:
            state = state_ref[j]
            norm = norm_ref[j][:, :1]
            moved = KEEP * momentum_ref[j] + total / scale
        state = state - RATE * moved
        state = state * (norm / norm_of(state))
        piece_ref[0, j] = state.astype(BF)
        if first:
            state_out[j] = state
            momentum_out[j] = moved
            norm_out[j] = jnp.broadcast_to(norm, norm_out.shape[1:])


def update(scale, own, recv, start=None, carried=None):
    first = start is not None
    operands = [scale, own, *recv] + ([start] if first else list(carried))
    outs = [((1,) + own.shape, BF), ((8, own.shape[1]), F32)]
    if first:
        outs += [(own.shape, F32), (own.shape, F32), (own.shape[:2] + (128,), F32)]
    return call(functools.partial(update_body, first, len(recv)), operands, 1, outs)


def write_payload(out_ref, totals, level):
    width = totals[0].shape[0]
    for j, total in enumerate(totals):
        out_ref[j * width : (j + 1) * width] = total.astype(BF)
    high = level.astype(BF).astype(F32)
    mid = (level - high).astype(BF).astype(F32)
    low = level - high - mid
    line = lax.broadcasted_iota(jnp.int32, level.shape, 0)
    terms = jnp.where(line == 0, high, jnp.where(line == 1, mid, jnp.where(line == 2, low, 0.0)))
    out_ref[len(totals) * width :] = terms.astype(BF)


def read_level(ref):
    terms = ref[ref.shape[0] - 8 :].astype(F32)
    return terms[0:1] + terms[1:2] + terms[2:3]


def pack_body(own_ref, one_ref, two_ref, three_ref, first_ref, second_ref, out_ref):
    totals = []
    for j in range(own_ref.shape[0]):
        total = own_ref[j]
        for ref in (one_ref, two_ref, three_ref):
            total = total + ref[j].astype(F32)
        totals.append(total)
    width = first_ref.shape[1]
    dim = own_ref.shape[2]
    gap = jnp.zeros((8, 128 - width), F32)
    rest = jnp.zeros((8, dim - 256), F32)
    level = jnp.concatenate([first_ref[...], gap, second_ref[...], gap, rest], axis=1)
    write_payload(out_ref, totals, level)


def pack(own, recv, first, second):
    n, width, dim = own.shape
    return call(pack_body, (own, *recv, first, second), 0, [((n * width + 8, dim), BF)])[0]


def sum_of(own_ref, recv, rows):
    one, two, three = [ref[rows].astype(F32) for ref in recv]
    return (own_ref[rows].astype(F32) + two) + (one + three)


def max_level(own_ref, recv):
    level = read_level(own_ref)
    for ref in recv:
        level = jnp.maximum(level, read_level(ref))
    return level


def mix_body(own_ref, one_ref, two_ref, three_ref, out_ref):
    recv = (one_ref, two_ref, three_ref)
    width = (own_ref.shape[0] - 8) // 3
    totals = [sum_of(own_ref, recv, slice(j * width, (j + 1) * width)) for j in range(3)]
    level = max_level(own_ref, recv)
    write_payload(out_ref, totals, jnp.broadcast_to(level, (8, level.shape[1])))


def mix(own, recv):
    return call(mix_body, (own, *recv), 0, [(own.shape, BF)])[0]


def finish_body(own_ref, one_ref, two_ref, three_ref, gate_ref, up_ref, down_ref, level_ref):
    recv = (one_ref, two_ref, three_ref)
    width = gate_ref.shape[0]
    for j, out in enumerate((gate_ref, up_ref, down_ref)):
        out[...] = sum_of(own_ref, recv, slice(j * width, (j + 1) * width))
    level = max_level(own_ref, recv)
    level_ref[0:1, :] = level[:, :width]
    level_ref[1:2, :] = level[:, 128 : 128 + width]


def finish(own, recv):
    rows, dim = own.shape
    width = (rows - 8) // 3
    outs = [((width, dim), F32)] * 3 + [((2, width), F32)]
    return call(finish_body, (own, *recv), 0, outs)


def per_device(
    keys, values, queries, token_rate, valid_count, loss_scale, w_gate, w_up, w_down, out_cotangent
):
    parts = lax.axis_size("tok")
    seqs = lax.axis_size("seq")
    chips = parts // 2
    side = math.isqrt(seqs)

    def z_shift(array, k):
        pairs = [(2 * z + c, 2 * ((z + k) % chips) + c) for z in range(chips) for c in range(2)]
        return lax.ppermute(array, "tok", pairs)

    def other_core(array):
        return lax.ppermute(array, "tok", [(t, t ^ 1) for t in range(parts)])

    def across(array, first):
        recv = []
        for k in range(1, side):
            pairs = []
            for t in range(parts):
                for y in range(side):
                    for x in range(side):
                        to = (y, (x + k) % side) if (t % 2 == 0) == first else ((y + k) % side, x)
                        pairs.append(((t * side + y) * side + x, (t * side + to[0]) * side + to[1]))
            recv.append(lax.ppermute(array, ("tok", "seq"), pairs))
        return recv

    def scatter(own, other):
        sums = combine(own, other_core(other), chips)
        recv = []
        for k in range(1, chips):
            recv.append(z_shift(sums[k], k))
        return sums[0], recv

    def spread(piece):
        mine = [piece] + [z_shift(piece, chips - k) for k in range(1, chips)]
        return mine, [other_core(p) for p in mine]

    half = w_gate.shape[1] // 2
    args = (valid_count, loss_scale, token_rate)
    other, x, e, first, _ = lead(
        keys, values, token_rate, w_gate, w_up, w_down, valid_count, loss_scale, parts
    )
    own = grads(True, 0, args, x, e, [first], F32)[0]
    own, recv = scatter(own, other)
    piece, level0, *carried = update(loss_scale, own, recv, start=first)
    halves = spread(piece)
    acc, done = grads(False, 0, args, queries, out_cotangent, halves[0] + halves[1], F32, result=True)
    other = grads(True, 1, args, keys, values, halves[1], BF)[0]
    own = grads(True, 1, args, keys, values, halves[0], F32)[0]
    own, recv = scatter(own, other)
    piece, level1 = update(loss_scale, own, recv, carried=carried)
    halves = spread(piece)
    other = grads(False, 1, args, queries, out_cotangent, halves[1], BF, acc=acc, skip=half)[0]
    own = grads(False, 1, args, queries, out_cotangent, halves[0], F32, acc=acc, skip=0)[0]
    own, recv = scatter(own, other)
    fast_out = output_of(valid_count, queries, done, halves[0] + halves[1])
    packed = pack(own, recv, level0, level1)
    packed = mix(packed, across(packed, True))
    gate, up, down, level = finish(packed, across(packed, False))
    return (fast_out, gate.T, up.T, down, level)


def solution(mesh):
    placed = (
        P("seq", None, "tok", None),
        P("seq", None, "tok", None),
        P("seq", None, "tok", None),
        P("seq", None, "tok"),
        P("seq", None),
        P(),
        P(),
        P(),
        P(),
        P("seq", None, "tok", None),
    )

    return jax.shard_map(
        per_device,
        mesh=mesh,
        in_specs=placed,
        out_specs=(
            P("seq", None, "tok", None),
            P(None, "tok"),
            P(None, "tok"),
            P("tok", None),
            P(None, "tok"),
        ),
        check_vma=False,
    )
```

```python
import functools
import math
import jax
import jax.numpy as jnp
from jax import lax
from jax.experimental import pallas as pl
from jax.experimental.pallas import tpu as pltpu
from jax.sharding import PartitionSpec as P


KEEP = 0.9
RATE = 3.0
TINY = 1e-06
BF = jnp.bfloat16
F32 = jnp.float32
NT = (((1,), (1,)), ((), ()))
TN = (((0,), (0,)), ((), ()))
MIB = 1024 * 1024
NEAR, FAR, OPPOSITE = MOVES = range(3)
TILE = 1024
LEAD_TILE = 512

GROUPS = (((0, 0), (0, 1), (0, 2)), ((1, 1), (1, 2)), ((1, 0), (1, 3), (0, 3)))


def dot(a, b, dims=None):
    if dims is None:
        return jnp.dot(a, b, preferred_element_type=F32)
    return lax.dot_general(a, b, dims, preferred_element_type=F32)


VMEM = pl.BlockSpec(memory_space=pltpu.VMEM)
SMEM = pl.BlockSpec(memory_space=pltpu.SMEM)
ANY = pl.BlockSpec(memory_space=pltpu.HBM)


def call(body, operands, n_smem, outs, scratch=(), limit=8, flops=0, n_exp=0, n_any=0):
    shapes = [jax.ShapeDtypeStruct(s, t) for s, t in outs]
    cost = None
    if flops:
        cost = pl.CostEstimate(flops=flops, transcendentals=n_exp, bytes_accessed=4 * MIB)
    return pl.pallas_call(
        body,
        in_specs=[ANY] * n_any + [SMEM] * n_smem + [VMEM] * (len(operands) - n_smem - n_any),
        out_specs=[VMEM] * len(shapes),
        out_shape=shapes,
        scratch_shapes=list(scratch),
        cost_estimate=cost,
        compiler_params=pltpu.CompilerParams(vmem_limit_bytes=limit * MIB),
    )(*operands)


def gather_rows(pieces, gu, down):
    k = 0
    rows = down.shape[0]
    for ref in pieces:
        n, _, width, _ = ref.shape
        for i in range(n):
            gu[k * width : (k + 1) * width] = ref[i, 0]
            gu[rows + k * width : rows + (k + 1) * width] = ref[i, 1]
            down[k * width : (k + 1) * width] = ref[i, 2]
            k += 1


def mask_row(count, start, size, tokens):
    base = lax.axis_index("tok") * tokens + start
    return base + lax.broadcasted_iota(jnp.int32, (1, size), 1) < count


def tile_grads(x, e, row, gu, down):
    rows = down.shape[0]
    ab = dot(gu[...], x, NT)
    a = ab[:rows]
    b = ab[rows:]
    r = dot(down[...], e, NT) * row
    s = 0.5 + 0.5 * jnp.tanh(0.5 * a)
    act = a * s
    hidden = (act * b * row).astype(BF)
    e_up = (r * act).astype(BF)
    e_gate = (r * b * (s + act * (1.0 - s))).astype(BF)
    return ((e_gate, x), (e_up, x), (hidden, e))


def add_grads(pairs, i, steps, acc, outs, starts=()):
    for j, (left, right) in enumerate(pairs):
        value = dot(left, right)
        if i > 0:
            value = value + acc[j]
        if i < steps - 1:
            acc[j] = value
            continue
        row = 0
        for n, out in enumerate(outs):
            slots, _, width, _ = out.shape
            for k in range(slots):
                part = value[row : row + width]
                if starts:
                    part = part + starts[n][k, j]
                out[k, j] = part.astype(out.dtype)
                row += width


def grad_scratch(n_rows, dim):
    return [pltpu.VMEM((2 * n_rows, dim), BF), pltpu.VMEM((n_rows, dim), BF), pltpu.VMEM((3, n_rows, dim), F32)]


def grad_cost(tokens, n_rows, dim):
    return dict(limit=28, flops=12 * tokens * n_rows * dim, n_exp=tokens * n_rows)


def lead_body(keys_ref, values_ref, rate_hbm, gate_hbm, up_hbm, down_hbm, count_hbm, scale_ref, *refs):
    outs = refs[:2]
    x_ref, e_ref, rows_ref, scale_out = refs[2:6]
    pieces = refs[6:9]
    gate_ref, up_ref, down_ref, gate_t, up_t, rate_ref, count_ref, gu, down, acc, sems = refs[9:]
    tokens = x_ref.shape[0]
    steps = tokens // LEAD_TILE
    spans = [slice(i * LEAD_TILE, (i + 1) * LEAD_TILE) for i in range(steps)]
    copies = [(gate_hbm, gate_ref), (up_hbm, up_ref), (down_hbm, down_ref)]
    copies += [(count_hbm, count_ref), (rate_hbm, rate_ref)]
    for span in spans:
        copies += [(keys_ref.at[0, 0, span], x_ref.at[span]), (values_ref.at[0, 0, span], e_ref.at[span])]
    copies = [pltpu.make_async_copy(a, b, sems.at[n]) for n, (a, b) in enumerate(copies)]
    for copy in copies:
        copy.start()
    where = lax.axis_index("tok")
    z = where // 2
    core = where % 2
    chips = 4
    width = pieces[0].shape[2]
    copies[0].wait()
    gate_t[...] = gate_ref[...].T
    copies[1].wait()
    up_t[...] = up_ref[...].T
    copies[2].wait()
    odd = (z + core) % 2
    near = (z + 1 + 2 * odd) % chips
    far = (z + 3 + 2 * odd) % chips
    order = ((z, near, far, (z + 2) % chips), (z, far, near, (z + 2) % chips))
    for out, group in zip(pieces, GROUPS):
        for i, (half, slot) in enumerate(group):
            owner = 2 * order[half][slot] + (core + half) % 2
            rows = pl.ds(pl.multiple_of(owner * width, width), width)
            out[i, 0] = gate_t[rows, :]
            out[i, 1] = up_t[rows, :]
            out[i, 2] = down_ref[rows, :]
    gather_rows(pieces[2:], gu, down)
    for n in range(3, 5):
        copies[n].wait()
    scale = scale_ref[0]
    scale_out[...] = jnp.full(scale_out.shape, scale, F32)
    for block in range(2):
        valid = mask_row(count_ref[0, block], 0, tokens, tokens)
        factor = -(scale / jnp.full((1, 1), count_ref[0, block], jnp.int32).astype(F32))
        rows_ref[block : block + 1] = jnp.where(valid, rate_ref[0, block : block + 1, :] * factor, 0.0)
        rows_ref[2 + block : 3 + block] = jnp.where(valid, 1.0, 0.0)
    for i, span in enumerate(spans):
        copies[5 + 2 * i].wait()
        copies[6 + 2 * i].wait()
        pairs = tile_grads(x_ref[span], e_ref[span], rows_ref[0:1, span], gu, down)
        add_grads(pairs, i, steps, acc, outs)


def lead(keys, values, rate, w_gate, w_up, w_down, count, scale, parts):
    tokens, dim = keys.shape[2:]
    hid = w_gate.shape[1]
    width = hid // parts
    shapes = [(len(group), 3, width, dim) for group in GROUPS]
    n_rows = shapes[2][0] * width
    outs = [((2, 3, width, dim), BF), ((1, 3, width, dim), F32)]
    outs += [((tokens, dim), BF), ((tokens, dim), BF), ((8, tokens), F32), ((8, 128), F32)]
    outs += [(shape, BF) for shape in shapes]
    scratch = [pltpu.VMEM(w.shape, BF) for w in (w_gate, w_up, w_down)]
    scratch += [pltpu.VMEM((hid, dim), BF)] * 2
    scratch += [pltpu.VMEM(rate.shape, F32), pltpu.SMEM(count.shape, jnp.int32)]
    scratch += grad_scratch(n_rows, dim) + [pltpu.SemaphoreType.DMA((5 + 2 * (tokens // LEAD_TILE),))]
    operands = (keys, values, rate, w_gate, w_up, w_down, count)
    operands = [pltpu.with_memory_space_constraint(array, pltpu.HBM) for array in operands] + [scale]
    return call(lead_body, operands, 1, outs, scratch, n_any=7, **grad_cost(tokens, n_rows, dim))


def grads_body(line, block, n_pieces, n_starts, n_outs, rows_ref, x_ref, e_ref, *refs):
    pieces = refs[:n_pieces]
    starts = refs[n_pieces : n_pieces + n_starts]
    outs = refs[n_pieces + n_starts : n_pieces + n_starts + n_outs]
    gu, down, acc = refs[-3:]
    gather_rows(pieces, gu, down)
    flat = len(x_ref.shape) == 2
    tokens = x_ref.shape[-2]
    steps = tokens // TILE
    for i in range(steps):
        span = slice(i * TILE, (i + 1) * TILE)
        x = x_ref[span] if flat else x_ref[0, block, span]
        e = e_ref[span] if flat else e_ref[0, block, span]
        add_grads(tile_grads(x, e, rows_ref[line : line + 1, span], gu, down), i, steps, acc, outs, starts)


def grads(inner, block, rows, x, e, pieces, outs, starts=()):
    tokens, dim = x.shape[-2:]
    n_rows = sum(p.shape[0] * p.shape[2] for p in pieces)
    width = pieces[0].shape[2]
    line = block if inner else 2 + block
    return call(
        functools.partial(grads_body, line, block, len(pieces), len(starts), len(outs)),
        [rows, x, e, *pieces, *starts],
        0,
        [((n, 3, width, dim), t) for n, t in outs],
        grad_scratch(n_rows, dim),
        **grad_cost(tokens, n_rows, dim),
    )


def output_body(block, n_pieces, n_done, rows_ref, x_ref, *refs):
    pieces = refs[:n_pieces]
    done = refs[n_pieces : n_pieces + n_done]
    out_ref, gu, down = refs[-3:]
    gather_rows(pieces, gu, down)
    rows = down.shape[0]
    tokens = x_ref.shape[2]
    for other, ref in enumerate(done):
        out_ref[0, other] = ref[...]
    for i in range(tokens // TILE):
        span = slice(i * TILE, (i + 1) * TILE)
        row = rows_ref[2 + block : 3 + block, span]
        ab = dot(gu[...], x_ref[0, block, span], NT)
        a = ab[:rows]
        s = 0.5 + 0.5 * jnp.tanh(0.5 * a)
        hidden = (a * s * ab[rows:] * row).astype(BF)
        value = dot(hidden, down[...], TN).astype(BF)
        if n_done:
            out_ref[0, block, span] = value
        else:
            out_ref[span] = value


def output_of(block, mask, x, pieces, done=()):
    tokens, dim = x.shape[2:]
    n_rows = sum(p.shape[0] * p.shape[2] for p in pieces)
    return call(
        functools.partial(output_body, block, len(pieces), len(done)),
        [mask, x, *pieces, *done],
        0,
        [(x.shape if done else (tokens, dim), BF)],
        scratch=[pltpu.VMEM((2 * n_rows, dim), BF), pltpu.VMEM((n_rows, dim), BF)],
        limit=16,
        flops=6 * tokens * n_rows * dim,
        n_exp=tokens * n_rows,
    )[0]


def combine_body(own_ref, other_ref, *outs):
    first = own_ref.shape[0] - len(outs)
    for k, out in enumerate(outs):
        out[0] = (own_ref[first + k] + other_ref[k].astype(F32)).astype(out.dtype)


def combine(own, other):
    outs = [((1,) + own.shape[1:], BF)] * other.shape[0]
    return call(combine_body, (own, other), 0, outs)


def combine_late_body(own_ref, opposite_ref, other_ref, keep_ref, send_ref):
    keep_ref[0] = own_ref[0] + other_ref[0].astype(F32)
    send_ref[0] = (opposite_ref[0] + other_ref[1].astype(F32)).astype(BF)


def combine_late(own, opposite, other):
    shape = (1,) + own.shape[1:]
    return call(combine_late_body, (own, opposite, other), 0, [(shape, F32), (shape, BF)])


def add_body(own_slot, other_slot, own_ref, other_ref, *refs):
    total = own_ref[own_slot] + other_ref[other_slot].astype(F32)
    for ref in refs[:-1]:
        total = total + ref[0].astype(F32)
    refs[-1][0] = total.astype(refs[-1].dtype)


def add(own, own_slot, other, other_slot, *more):
    body = functools.partial(add_body, own_slot, other_slot)
    return call(body, (own, other, *more), 0, [((1,) + own.shape[1:], BF)])[0]


def near_body(own_ref, other_ref, late_ref, keep_ref, send_ref):
    keep_ref[0] = own_ref[0] + late_ref[0].astype(F32)
    send_ref[0] = (own_ref[1] + other_ref[0].astype(F32)).astype(BF)


def keep_and_near(own, other, late):
    shape = (1,) + own.shape[1:]
    return call(near_body, (own, other, late), 0, [(shape, F32), (shape, BF)])


def norm_of(w):
    return jnp.sqrt(jnp.sum(w * w, axis=1, keepdims=True) + TINY)


def update_body(first, n_recv, scale_ref, own_ref, *refs):
    recv = refs[:n_recv]
    refs = refs[n_recv:]
    if first:
        start_ref, piece_ref, level_ref, state_out, momentum_out, norm_out = refs
    else:
        state_ref, momentum_ref, norm_ref, piece_ref, level_ref = refs
    scale = scale_ref[0:1, 0:1]
    for j in range(3):
        total = own_ref[0, j]
        for ref in recv:
            total = total + ref[0, j].astype(F32)
        if j == 0:
            level = jnp.max(jnp.abs(total), axis=1, keepdims=True)
            level = jnp.broadcast_to(level, (level.shape[0], 128)).T
            level_ref[...] = level[: level_ref.shape[0]]
        if first:
            state = start_ref[0, j].astype(F32)
            norm = norm_of(state)
            moved = total / scale
        else:
            state = state_ref[j]
            norm = norm_ref[j][:, :1]
            moved = KEEP * momentum_ref[j] + total / scale
        state = state - RATE * moved
        state = state * (norm / norm_of(state))
        piece_ref[0, j] = state.astype(BF)
        if first:
            state_out[j] = state
            momentum_out[j] = moved
            norm_out[j] = jnp.broadcast_to(norm, norm_out.shape[1:])


def update(scale, own, recv, start=None, carried=None):
    first = start is not None
    operands = [scale, own, *recv] + ([start] if first else list(carried))
    shape = own.shape[1:]
    outs = [(own.shape, BF), ((8, shape[1]), F32)]
    if first:
        outs += [(shape, F32), (shape, F32), (shape[:2] + (128,), F32)]
    return call(functools.partial(update_body, first, len(recv)), operands, 0, outs)


def write_payload(out_ref, totals, level):
    width = totals[0].shape[0]
    for j, total in enumerate(totals):
        out_ref[j * width : (j + 1) * width] = total.astype(BF)
    high = level.astype(BF).astype(F32)
    mid = (level - high).astype(BF).astype(F32)
    low = level - high - mid
    line = lax.broadcasted_iota(jnp.int32, level.shape, 0)
    terms = jnp.where(line == 0, high, jnp.where(line == 1, mid, jnp.where(line == 2, low, 0.0)))
    out_ref[len(totals) * width :] = terms.astype(BF)


def read_level(ref):
    terms = ref[ref.shape[0] - 8 :].astype(F32)
    return terms[0:1] + terms[1:2] + terms[2:3]


def pack_body(own_ref, one_ref, two_ref, three_ref, first_ref, second_ref, out_ref):
    totals = []
    for j in range(3):
        total = own_ref[0, j]
        for ref in (one_ref, two_ref, three_ref):
            total = total + ref[0, j].astype(F32)
        totals.append(total)
    width = first_ref.shape[1]
    dim = own_ref.shape[3]
    gap = jnp.zeros((8, 128 - width), F32)
    rest = jnp.zeros((8, dim - 256), F32)
    level = jnp.concatenate([first_ref[...], gap, second_ref[...], gap, rest], axis=1)
    write_payload(out_ref, totals, level)


def pack(own, recv, first, second):
    _, n, width, dim = own.shape
    return call(pack_body, (own, *recv, first, second), 0, [((n * width + 8, dim), BF)])[0]


def sum_of(own_ref, recv, rows):
    near, far, opposite = [ref[rows].astype(F32) for ref in recv]
    return (own_ref[rows].astype(F32) + opposite) + (near + far)


def max_level(own_ref, recv):
    level = read_level(own_ref)
    for ref in recv:
        level = jnp.maximum(level, read_level(ref))
    return level


def mix_body(own_ref, one_ref, two_ref, three_ref, out_ref):
    recv = (one_ref, two_ref, three_ref)
    width = (own_ref.shape[0] - 8) // 3
    totals = [sum_of(own_ref, recv, slice(j * width, (j + 1) * width)) for j in range(3)]
    level = max_level(own_ref, recv)
    write_payload(out_ref, totals, jnp.broadcast_to(level, (8, level.shape[1])))


def mix(own, recv):
    return call(mix_body, (own, *recv), 0, [(own.shape, BF)])[0]


def finish_body(own_ref, one_ref, two_ref, three_ref, gate_ref, up_ref, down_ref, level_ref):
    recv = (one_ref, two_ref, three_ref)
    width = gate_ref.shape[0]
    for j, out in enumerate((gate_ref, up_ref, down_ref)):
        out[...] = sum_of(own_ref, recv, slice(j * width, (j + 1) * width))
    level = max_level(own_ref, recv)
    level_ref[0:1, :] = level[:, :width]
    level_ref[1:2, :] = level[:, 128 : 128 + width]


def finish(own, recv):
    rows, dim = own.shape
    width = (rows - 8) // 3
    outs = [((width, dim), F32)] * 3 + [((2, width), F32)]
    return call(finish_body, (own, *recv), 0, outs)


def per_device(
    keys, values, queries, token_rate, valid_count, loss_scale, w_gate, w_up, w_down, out_cotangent
):
    parts = lax.axis_size("tok")
    seqs = lax.axis_size("seq")
    chips = parts // 2
    side = math.isqrt(seqs)

    def other_core(array):
        return lax.ppermute(array, "tok", [(t, t ^ 1) for t in range(parts)])

    def neighbour(at, move):
        if move == OPPOSITE:
            return (at + 2) % 4
        return (at + 1) % 4 if (at % 2 == 0) == (move == NEAR) else (at + 3) % 4

    def across(array, first):
        recv = []
        for move in MOVES:
            pairs = []
            for t in range(parts):
                for y in range(side):
                    for x in range(side):
                        along_x = (t % 2 == 0) == first
                        to = (y, neighbour(x, move)) if along_x else (neighbour(y, move), x)
                        pairs.append(((t * side + y) * side + x, (t * side + to[0]) * side + to[1]))
            recv.append(lax.ppermute(array, ("tok", "seq"), pairs))
        return recv

    def z_swap(array, move):
        other = (FAR, NEAR, OPPOSITE)
        pairs = []
        for z in range(chips):
            pairs.append((2 * z, 2 * neighbour(z, move)))
            pairs.append((2 * z + 1, 2 * neighbour(z, other[move]) + 1))
        return lax.ppermute(array, "tok", pairs)

    def total_of(own, other, late):
        recv = []
        own = own()
        other = other()
        other = other_core(other)
        send = combine(own, other)
        for move, part in zip(MOVES, send):
            recv.append(z_swap(part, move))
        other, opposite = late()
        other = other_core(other)
        keep, send = combine_late(own, opposite, other)
        recv.append(z_swap(send, OPPOSITE))
        return keep, recv

    def first_total(rest, late, opposite):
        late = other_core(late)
        own, other = rest()
        other = other_core(other)
        send = add(opposite, 0, late, 1)
        passed = z_swap(send, NEAR)
        keep, send = keep_and_near(own, other, late)
        near = z_swap(send, NEAR)
        send = add(own, 2, other, 1, passed)
        far = z_swap(send, FAR)
        return keep, [near, far]

    def spread(piece):
        mine = [piece]
        for move in MOVES[:2]:
            mine.append(z_swap(piece, move))
        mine.append(z_swap(mine[2], NEAR))
        passed = []
        for array in mine:
            passed.append(other_core(array))
        return [[(mine, passed)[half][slot] for half, slot in group] for group in GROUPS]

    def group_grads(inner, block, x, e, groups, starts=None):
        def run(n, outs):
            start = () if starts is None else starts[n]
            return grads(inner, block, rows, x, e, groups[n], outs, start)

        return (
            lambda: run(0, [(3, F32)])[0],
            lambda: run(1, [(2, BF)])[0],
            lambda: run(2, [(2, BF), (1, F32)]),
        )

    late, opposite, x, e, rows, scale, *start = lead(
        keys, values, token_rate, w_gate, w_up, w_down, valid_count, loss_scale, parts
    )
    rest = lambda: grads(True, 0, rows, x, e, start[:2], [(3, F32), (2, BF)])
    total, recv = first_total(rest, late, opposite)
    piece, level0, *carried = update(scale, total, recv, start=start[0])
    groups = spread(piece)
    every = groups[0] + groups[1] + groups[2]
    outs = [(3, F32), (2, F32), (2, F32), (1, F32)]
    acc = grads(False, 0, rows, queries, out_cotangent, every, outs)
    done = output_of(0, rows, queries, every)
    total, recv = total_of(*group_grads(True, 1, keys, values, groups))
    piece, level1 = update(scale, total, recv, carried=carried)
    groups = spread(piece)
    starts = (acc[:1], acc[1:2], acc[2:])
    total, recv = total_of(*group_grads(False, 1, queries, out_cotangent, groups, starts))
    fast_out = output_of(1, rows, queries, groups[0] + groups[1] + groups[2], done=(done,))
    packed = pack(total, recv, level0, level1)
    recv = across(packed, True)
    packed = mix(packed, recv)
    recv = across(packed, False)
    gate, up, down, level = finish(packed, recv)
    return (fast_out, gate.T, up.T, down, level)


def solution(mesh):
    placed = (
        P("seq", None, "tok", None),
        P("seq", None, "tok", None),
        P("seq", None, "tok", None),
        P("seq", None, "tok"),
        P("seq", None),
        P(),
        P(),
        P(),
        P(),
        P("seq", None, "tok", None),
    )

    return jax.shard_map(
        per_device,
        mesh=mesh,
        in_specs=placed,
        out_specs=(
            P("seq", None, "tok", None),
            P(None, "tok"),
            P(None, "tok"),
            P("tok", None),
            P(None, "tok"),
        ),
        check_vma=False,
    )
```
